256 devices in a mesh: seq: 16 (over z, core), tp: 8 (over x_lo, y), dp: 2 (over x_hi).
Axes of the slice: x: 4 (x_hi: 2, x_lo: 2; x = x_hi * 2 + x_lo), y: 4, z: 8, core: 2. Of those that a mesh axis runs over, the one named last changes fastest.
Arguments:
- query_latent: bfloat16 [2, 4096, 1536], P('dp', 'seq', 'tp'), may hold values from -6 to 6
- key_latent: bfloat16 [2, 4096, 512], P('dp', 'seq', 'tp'), may hold values from -6 to 6
- rope_key: bfloat16 [2, 4096, 64], P('dp', 'seq'), may hold values from -6 to 6
- w_uq: bfloat16 [1536, 12288], P('seq', 'tp')
- w_uk: bfloat16 [512, 8192], P('seq', 'tp'), may hold values from -0.25 to 0.25
- w_uv: bfloat16 [512, 8192], P('seq', 'tp'), may hold values from -0.25 to 0.25
- block_order: int32 [2, 32], P('dp'), may hold values from 0 to 31, each once within a row
- segment_ids: int32 [2, 4096], P('dp'), may hold values from 0 to 3, never falling along the last dimension, each value on 1 to 2048 neighbouring positions
Outputs:
- context: bfloat16 [2, 4096, 8192], P('dp', 'seq', 'tp')
- clipped_uq: bfloat16 [1536, 12288], P('seq', 'tp')
- clipped_uk: bfloat16 [512, 8192], P('seq', 'tp')
The draws below stay inside these ranges and needn't reach their ends.
Inputs may be any that keep to these rules, and one draw needn't show every extreme that they name: `block_order`: each row is a permutation of the 32 position blocks. `segment_ids`: never falling along positions; each document has at most 2048 positions.
All inputs are finite; a program needn't handle non-finite values.
Results may differ from the reference program's by a relative error of at most 0.012.
The reference program's roundings to bfloat16 on the way (of `weights`) count: a program that leaves them out, or rounds other values in their place, can miss the bound.
Values may be sent and summed in bfloat16 or wider, within the bound.
A program may use at most 64 MiB of HBM per device.

```python
import math
import jax
import jax.numpy as jnp
import numpy as np
from jax import lax

HEADS = 64
NOPE = 128
ROPE = 64
VD = 128
QL = 1536
KL = 512
TOK_DEV = 256
CLIP = 8
L = 4096
BLOCKS = 32
SEQS = 2
N_DP = 2


def draw_w_uq(key, part):
    first, second = jax.random.split(jax.random.fold_in(key, 11))
    base = jax.random.normal(first, (QL, HEADS * (NOPE + ROPE)), jnp.float32) * QL ** (-0.5)
    lowest, highest = (math.log(0.5), math.log(3.0))
    exponent = jax.random.uniform(second, (HEADS,), jnp.float32, lowest, highest)
    factor = jnp.repeat(jnp.exp(exponent), NOPE + ROPE)
    return (base * factor[None, :]).astype(jnp.bfloat16)


def shard_levels(stream_key, shape, pieces, least, top_value):
    def one(axis_at, blocks):
        draws = jax.random.uniform(jax.random.fold_in(jax.random.fold_in(stream_key, 6), axis_at), (blocks,), jnp.float32, least / len(pieces), top_value / len(pieces))
        return jnp.repeat(jnp.exp(draws), shape[axis_at] // blocks).reshape((-1,) + (1,) * (len(shape) - axis_at - 1))

    level = one(*pieces[0])
    for cut in pieces[1:]:
        level = level * one(*cut)
    return level


def length_profile(amount, total, reach, slope):
    portions = [(1 << 20) // math.isqrt(rank ** slope) + 1 for rank in range(2, amount + 1)]
    rest, counts = total - reach - (amount - 1), [1] * (amount - 1)
    while rest > 0:
        free = [i for i in range(amount - 1) if counts[i] < reach]
        pool, remaining = sum([portions[i] for i in free]), rest
        for i in free:
            extra = min(reach - counts[i], max(1, remaining * portions[i] // pool), rest)
            counts[i] = counts[i] + extra
            rest = rest - extra
    return np.array([reach] + counts)


def ragged(own_key, number_of, total, limit, slope):
    if number_of == 2:
        one = jax.random.randint(own_key, (), max(1, total - limit), min(limit, total - 1) + 1)
        return jnp.stack([one, total - one])
    lengths = jnp.asarray(length_profile(number_of, total, limit, slope), jnp.int32)
    twos = (number_of - 1) // 2
    giver, taker = lengths[1:1 + 2 * twos:2], lengths[2:2 + 2 * twos:2]
    room = jnp.minimum(giver - 1, limit - taker)
    moved = jax.random.randint(jax.random.fold_in(own_key, 1), (twos,), 0, 1 << 20) % (room + 1)
    lengths = lengths.at[1:1 + 2 * twos:2].set(giver - moved).at[2:2 + 2 * twos:2].set(taker + moved)
    return lengths[jax.random.permutation(jax.random.fold_in(own_key, 2), number_of)]


def centred(rng, extent, deviation, bound, cuts=(), kind=jnp.bfloat16):
    level = shard_levels(rng, extent, cuts, -0.22, 0.18) if cuts else 1.0
    drawn = jax.random.normal(rng, extent, jnp.float32) * deviation * level
    return jnp.minimum(jnp.maximum(drawn, -bound), bound).astype(kind)


def setup_inputs(seed: int = 0) -> dict:
    splits = jax.random.split(jax.random.key(seed), 9)
    query_latent = centred(splits[0], (SEQS, L, QL), 1.0, 6.0, ((0, 2), (1, 16), (2, 8)))
    key_latent = centred(splits[1], (SEQS, L, KL), 1.0, 6.0, ((0, 2), (1, 16), (2, 8)))
    rope_key = centred(splits[2], (SEQS, L, ROPE), 1.0, 6.0, ((0, 2), (1, 16)))
    w_uq = draw_w_uq(jax.random.fold_in(splits[8], 71), 0)
    w_uk = centred(splits[4], (KL, HEADS * NOPE), KL ** -0.5, 0.25, ((0, 16), (1, 8)))
    w_uv = centred(splits[5], (KL, HEADS * VD), KL ** -0.5, 0.25, ((0, 16), (1, 8)))
    block_order = jax.vmap(lambda own: jax.random.permutation(own, BLOCKS))(jax.random.split(splits[6], SEQS)).reshape((SEQS, BLOCKS)).astype(jnp.int32)
    segment_ids = jax.vmap(lambda own: jnp.searchsorted(jnp.cumsum(ragged(own, 4, L, L // 2, 1)), jnp.arange(L), side="right"))(jax.random.split(splits[7], SEQS)).reshape((SEQS, L)).astype(jnp.int32)
    return {"query_latent": query_latent, "key_latent": key_latent, "rope_key": rope_key, "w_uq": w_uq, "w_uk": w_uk, "w_uv": w_uv, "block_order": block_order, "segment_ids": segment_ids}


rope_base = 50000.0
masked_value = -1e+30

def turning(positions, width):
    steps = jnp.arange(width // 2, dtype=jnp.float32) * (2.0 / width)
    freqs = jnp.exp(-math.log(rope_base) * steps)
    angle = positions.astype(jnp.float32)[:, None] * freqs[None, :]
    return (jnp.cos(angle), jnp.sin(angle))

def rotate(values, cosine, sine):
    half = values.shape[-1] // 2
    first = values[..., :half]
    second = values[..., half:]
    return jnp.concatenate([first * cosine - second * sine, second * cosine + first * sine], axis=-1)

def stored_positions(order, half_block):
    count = order.shape[0] * half_block
    index = jnp.arange(count, dtype=jnp.int32)
    return (jnp.take(order, index // half_block) * half_block + index % half_block).astype(jnp.int32)

def reference(query_latent, key_latent, rope_key, w_uq, w_uk, w_uv, block_order, segment_ids):
    half_block = TOK_DEV // 2
    scale = 1.0 / math.sqrt(NOPE + ROPE)
    contexts = []
    largest = jnp.full((HEADS,), masked_value, jnp.float32)
    for member in range(N_DP):
        positions = stored_positions(block_order[member], half_block)
        labels = jnp.take(segment_ids[member], positions)
        cosine, sine = turning(positions, ROPE)
        query_full = jnp.dot(query_latent[member], w_uq, preferred_element_type=jnp.float32).reshape(L, HEADS, NOPE + ROPE)
        query_nope = query_full[:, :, :NOPE].astype(jnp.bfloat16)
        query_rope = rotate(query_full[:, :, NOPE:], cosine[:, None, :], sine[:, None, :]).astype(jnp.bfloat16)
        key_nope = jnp.dot(key_latent[member], w_uk, preferred_element_type=jnp.float32).astype(jnp.bfloat16).reshape(L, HEADS, NOPE)
        values = jnp.dot(key_latent[member], w_uv, preferred_element_type=jnp.float32).astype(jnp.bfloat16).reshape(L, HEADS, VD)
        key_rope = rotate(rope_key[member].astype(jnp.float32), cosine, sine).astype(jnp.bfloat16)
        allowed = (positions[None, :] <= positions[:, None]) & (labels[None, :] == labels[:, None])

        def one_head(inputs):
            head_qn, head_qr, head_kn, head_values = inputs
            scores = jnp.dot(head_qn, head_kn.T, preferred_element_type=jnp.float32)
            scores = (scores + jnp.dot(head_qr, key_rope.T, preferred_element_type=jnp.float32)) * scale
            masked = jnp.where(allowed, scores, masked_value)
            row_max = lax.optimization_barrier(jnp.max(masked, axis=1))
            weights = jnp.where(allowed, jnp.exp(masked - row_max[:, None]), 0.0)
            total = lax.optimization_barrier(jnp.sum(weights, axis=1))
            mixed = jnp.dot(weights.astype(jnp.bfloat16), head_values, preferred_element_type=jnp.float32)
            return ((mixed / total[:, None]).astype(jnp.bfloat16), jnp.max(row_max))
        per_head, head_max = lax.map(one_head, (jnp.transpose(query_nope, (1, 0, 2)), jnp.transpose(query_rope, (1, 0, 2)), jnp.transpose(key_nope, (1, 0, 2)), jnp.transpose(values, (1, 0, 2))))
        contexts.append(jnp.transpose(per_head, (1, 0, 2)).reshape(L, HEADS * VD))
        largest = jnp.maximum(largest, head_max)
    ratio = CLIP / jnp.maximum(largest, CLIP)
    root = jnp.sqrt(ratio)
    factors = jnp.concatenate([jnp.broadcast_to(root[:, None], (HEADS, NOPE)), jnp.broadcast_to(ratio[:, None], (HEADS, ROPE))], axis=1).reshape(HEADS * (NOPE + ROPE))
    clipped_uq = (w_uq.astype(jnp.float32) * factors[None, :]).astype(jnp.bfloat16)
    clipped_uk = (w_uk.astype(jnp.float32) * jnp.repeat(root, NOPE)[None, :]).astype(jnp.bfloat16)
    return (jnp.stack(contexts), clipped_uq, clipped_uk)
```

```python
import functools
import math

import jax
import jax.numpy as jnp
from jax import lax
from jax.experimental import pallas as pl
from jax.experimental.pallas import tpu as pltpu
from jax.sharding import PartitionSpec as P

NOPE = 128
ROPE = 64
VD = 128
CLIP = 8
NZ = 8
NY = 4
NX = 2
NTP = NX * NY
BLK = 128
MIB = 1 << 20

rope_base = 50000.0
masked_value = -1e30
MESH = pl.DeviceIdType.MESH
F32 = jnp.float32
BF16 = jnp.bfloat16


def cos_sin(angle):
    k = jnp.floor(angle * (2.0 / math.pi) + 0.5)
    r = angle - k * 1.5703125
    r = r - k * 4.837512969970703125e-4
    r = r - k * 7.54978995489188216e-8
    z = r * r
    s = ((-1.9515295891e-4 * z + 8.3321608736e-3) * z - 1.6666654611e-1) * z * r + r
    c = (
        ((2.443315711809948e-5 * z - 1.388731625493765e-3) * z + 4.166664568298827e-2) * z * z
        - 0.5 * z
        + 1.0
    )
    q = k - 4.0 * jnp.floor(k * 0.25)
    odd = (q == 1.0) | (q == 3.0)
    sine = jnp.where(odd, c, s)
    cosine = jnp.where(odd, s, c)
    sine = jnp.where(q >= 2.0, -sine, sine)
    cosine = jnp.where((q == 1.0) | (q == 2.0), -cosine, cosine)
    return cosine, sine


def turning(pos, lane):
    step = lax.rem(lane, ROPE // 2).astype(F32) * (2.0 / ROPE)
    freq = jnp.exp(-math.log(rope_base) * step)
    cosine, sine = cos_sin(pos.astype(F32) * freq)
    sine = jnp.where(lax.rem(lane, ROPE) < ROPE // 2, -sine, sine)
    return cosine, sine


def swapped(x):
    h = ROPE // 2
    return jnp.concatenate(
        [x[:, h : 2 * h], x[:, :h], x[:, 3 * h : 4 * h], x[:, 2 * h : 3 * h]], axis=1
    )


def folded(x):
    n = x.shape[0] // 2
    return jnp.concatenate([x[:n], x[n:]], axis=1)


def gather_kernel(
    order, rope_ref, key_ref, query_hbm, uq_hbm, uk_hbm, uv_hbm,
    k_out, vt_out, kr_out, q_out,
    wq, wk, wv, lp, rr, qg, wvt, trig, ssem, rsem, lsem,
):
    seq = lax.axis_index("seq")
    tp = lax.axis_index("tp")
    z, c = seq // 2, lax.rem(seq, 2)
    x, y = tp // NY, lax.rem(tp, NY)
    oc = 1 - c

    def zmod(d):
        return lax.rem(z + (d + NZ), NZ)

    def col(dx, dy):
        return (x if dx == 0 else 1 - x) * NY + lax.rem(y + (dy + NY), NY)

    right = {"seq": zmod(1) * 2 + c}
    left = {"seq": zmod(-1) * 2 + c}
    sibling = {"seq": z * 2 + oc}
    xside = {"tp": col(1, 0)}
    yup = {"tp": col(0, 1)}
    ydown = {"tp": col(0, -1)}
    offs = (0, -1, 1, -2, 2, -3, 3, 4)

    local = [
        pltpu.make_async_copy(query_hbm.at[0], qg.at[tp], lsem.at[0]),
        pltpu.make_async_copy(uk_hbm, wk.at[seq], lsem.at[1]),
        pltpu.make_async_copy(uv_hbm, wv.at[seq], lsem.at[2]),
        pltpu.make_async_copy(uq_hbm, wq.at[seq], lsem.at[3]),
    ]
    for cp in local:
        cp.start()
    barrier = pltpu.get_barrier_semaphore()
    for peer in (right, left, sibling, xside, yup, ydown):
        pl.semaphore_signal(barrier, inc=1, device_id=peer, device_id_type=MESH)

    lp[tp, c, 0] = folded(key_ref[0])
    lane = lax.broadcasted_iota(jnp.int32, (BLK, 2 * ROPE), 1)
    row = lax.broadcasted_iota(jnp.int32, (BLK, 2 * ROPE), 0)
    p0, p1 = order[0, 2 * seq] * BLK, order[0, 2 * seq + 1] * BLK
    kpos = row + jnp.where(lane < ROPE, p0, p1)
    cosine, sine = turning(kpos, lane)
    raw = folded(rope_ref[0].astype(F32))
    rr[c, z] = (raw * cosine + swapped(raw) * sine).astype(BF16)
    for b, p in ((0, p0), (1, p1)):
        cosine, sine = turning(row + p, lane)
        trig[0, b * BLK : (b + 1) * BLK] = cosine
        trig[1, b * BLK : (b + 1) * BLK] = sine

    sends = []
    names = {}

    def sem_of(key):
        if key not in names:
            names[key] = len(names)
        return rsem.at[names[key]]

    def send(src, dst, key, peer):
        cp = pltpu.make_async_remote_copy(
            src_ref=src, dst_ref=dst, send_sem=ssem.at[len(sends)], recv_sem=sem_of(key),
            device_id=peer, device_id_type=MESH,
        )
        cp.start()
        sends.append(cp)

    def arrived(ref, key):
        pltpu.make_async_remote_copy(
            src_ref=ref, dst_ref=ref, send_sem=ssem.at[0], recv_sem=sem_of(key),
            device_id=sibling, device_id_type=MESH,
        ).wait_recv()

    half = wq.shape[1] // 2

    def piece(item, sid, core):
        zs = zmod(offs[sid])
        if item == "l":
            return lp.at[tp, core, sid]
        if item == "r":
            return rr.at[core, zs]
        if item == "k":
            return wk.at[zs * 2 + core]
        if item == "v":
            return wv.at[zs * 2 + core]
        return wq.at[zs * 2 + core, pl.ds(half * int(item[1]), half)]

    def moved(item, sid, going):
        if item == "l":
            nxt = {0: 1, 1: 3, 3: 5, 5: 7} if going == "r" else {0: 2, 2: 4, 4: 6, 6: 7}
            return lp.at[tp, c, nxt[sid]], nxt[sid]
        nxt = {0: 1, 1: 3, 3: 5, 5: 7} if going == "r" else {0: 2, 2: 4, 4: 6, 6: 7}
        return piece(item, sid, c), nxt[sid]

    by_right = ("l", "r", "k", "q0")

    def pass_on(item, sid):
        src = piece(item, sid, c)
        if sid in (0, 1, 3) or (sid == 5 and item in by_right):
            dst, n = moved(item, sid, "r")
            send(src, dst, ("ring", item, n), right)
        if sid in (0, 2, 4) or (sid == 6 and item not in by_right):
            dst, n = moved(item, sid, "l")
            send(src, dst, ("ring", item, n), left)
        send(src, src, ("sib", item, sid), sibling)

    def ring(item, *sids):
        for sid in sids:
            arrived(piece(item, sid, c), ("ring", item, sid))
            pass_on(item, sid)

    def part(item, column, core=None):
        if item == "Q":
            return qg.at[column]
        return lp.at[column, c if core is None else core, pl.ds(2 * item, 2)]

    def share(item, column, name):
        if item != "Q":
            ref = part(item, column)
            send(ref, ref, ("share", item, name), sibling)

    def plane_own(item):
        ref = part(item, tp)
        send(ref, ref, ("x", item), xside)
        send(ref, ref, ("up", item, 0), yup)
        send(ref, ref, ("down", item, 0), ydown)

    def plane_x(item):
        ref = part(item, col(1, 0))
        arrived(ref, ("x", item))
        send(ref, ref, ("up", item, 1), yup)
        send(ref, ref, ("down", item, 1), ydown)
        share(item, col(1, 0), "x")

    def plane_y(item):
        for k in (0, 1):
            ref = part(item, col(k, -1))
            arrived(ref, ("up", item, k))
            if k == 0:
                send(ref, ref, ("far", item, 0), yup)
            share(item, col(k, -1), ("up", k))
            ref = part(item, col(k, 1))
            arrived(ref, ("down", item, k))
            if k == 1:
                send(ref, ref, ("far", item, 1), ydown)
            share(item, col(k, 1), ("down", k))

    def plane_far(item):
        for k in (0, 1):
            arrived(part(item, col(k, 2)), ("far", item, k))
            share(item, col(k, 2), ("far", k))

    def from_sibling(item):
        for sid in range(NZ):
            arrived(piece(item, sid, oc), ("sib", item, sid))

    def shared(item):
        arrived(part(item, col(1, 0), oc), ("share", item, "x"))
        for k in (0, 1):
            arrived(part(item, col(k, -1), oc), ("share", item, ("up", k)))
            arrived(part(item, col(k, 1), oc), ("share", item, ("down", k)))
            arrived(part(item, col(k, 2), oc), ("share", item, ("far", k)))

    def project(group):
        def one(i, carry):
            core = i // 2
            sid = 2 * group + lax.rem(i, 2)
            d = (sid + 1) // 2
            away = jnp.where(lax.rem(sid, 2) == 0, d, NZ - d)
            zs = lax.rem(z + away, NZ)
            low, high = [], []
            for pair in range(NTP // 2):
                a, b = lp[2 * pair, core, sid], lp[2 * pair + 1, core, sid]
                low.append(jnp.concatenate([a[:, :64], b[:, :64]], axis=1))
                high.append(jnp.concatenate([a[:, 64:], b[:, 64:]], axis=1))
            latent = jnp.concatenate(
                [jnp.concatenate(low, axis=1), jnp.concatenate(high, axis=1)], axis=0
            )
            first = pl.multiple_of((zs * 2 + core) * 256, 256)
            weight = wk[...].reshape(-1, wk.shape[2])
            k_out[pl.ds(first, 256), :] = jnp.dot(
                latent, weight, preferred_element_type=F32
            ).astype(BF16)
            vt_out[:, pl.ds(first, 256)] = lax.dot_general(
                wvt[...], latent, (((1,), (1,)), ((), ())), preferred_element_type=F32
            ).astype(BF16)
            rot = rr[core, zs]
            kr_out[pl.ds(first, BLK), :] = jnp.concatenate([rot[:, :64], rot[:, :64]], axis=1)
            kr_out[pl.ds(first + BLK, BLK), :] = jnp.concatenate([rot[:, 64:], rot[:, 64:]], axis=1)
            return carry

        lax.fori_loop(0, 4, one, 0)

    pl.semaphore_wait(barrier, 6)
    for item in ("l", "r"):
        pass_on(item, 0)
    local[0].wait()
    plane_own("Q")
    local[1].wait()
    local[2].wait()
    for item in ("k", "v"):
        pass_on(item, 0)
    local[3].wait()
    ring("l", 1, 2)
    ring("r", 1, 2)
    plane_own(0)
    plane_x("Q")
    ring("k", 1, 2)
    ring("v", 1, 2)
    for item in ("q0", "q1"):
        pass_on(item, 0)
    ring("l", 3, 4)
    ring("r", 3, 4)
    plane_own(1)
    plane_x(0)
    plane_y("Q")
    ring("k", 3, 4)
    ring("v", 3, 4)
    ring("l", 5, 6)
    ring("r", 5, 6)
    plane_own(2)
    plane_x(1)
    ring("q0", 1, 2)
    ring("q1", 1, 2)
    plane_y(0)
    ring("l", 7)
    ring("r", 7)
    plane_own(3)
    plane_x(2)
    plane_far("Q")
    ring("k", 5, 6)
    ring("v", 5, 6)
    plane_y(1)
    plane_far(0)
    plane_x(3)
    ring("k", 7)
    ring("v", 7)
    ring("q0", 3, 4)
    ring("q1", 3, 4)
    plane_y(2)
    plane_far(1)
    for item in ("l", "r", "k", "v"):
        from_sibling(item)
    wvt[...] = wv[...].reshape(-1, wv.shape[2]).astype(F32).T.astype(BF16)
    shared(0)
    project(0)
    plane_y(3)
    plane_far(2)
    ring("q0", 5, 6)
    ring("q1", 5, 6)
    shared(1)
    project(1)
    plane_far(3)
    shared(2)
    project(2)
    ring("q0", 7)
    ring("q1", 7)
    shared(3)
    project(3)
    from_sibling("q0")
    from_sibling("q1")

    rows_q = wq.shape[1] * 2

    def heads_pair(pair, carry):
        cols = pl.ds(pl.multiple_of(pair * 384, 128), 384)
        acc = jnp.zeros((256, 384), F32)
        for t in range(NTP):
            acc = acc + jnp.dot(
                qg[t],
                wq[2 * t : 2 * t + 2, :, cols].reshape(rows_q, 384),
                preferred_element_type=F32,
            )
        t0, t1, t2 = acc[:, :128], acc[:, 128:256], acc[:, 256:]
        at = lax.broadcasted_iota(jnp.int32, (256, 128), 1)
        rope = jnp.where(at < ROPE, t1, t2)
        rope = rope * trig[0] + swapped(rope) * trig[1]
        nope1 = jnp.concatenate([t1[:, 64:], t2[:, :64]], axis=1)
        q_out[2 * pair, :, :128] = t0.astype(BF16)
        q_out[2 * pair, :, 128:] = jnp.where(at < ROPE, rope, 0.0).astype(BF16)
        q_out[2 * pair + 1, :, :128] = nope1.astype(BF16)
        q_out[2 * pair + 1, :, 128:] = jnp.where(at < ROPE, 0.0, rope).astype(BF16)
        return carry

    lax.fori_loop(0, 4, heads_pair, 0)
    for cp in sends:
        cp.wait_send()


def attention_kernel(order, segs, seg_rows, q_ref, k_ref, vt_ref, kr_ref, out_ref, max_ref, inv, acc, m_ref, l_ref):
    heads = q_ref.shape[0]
    blocks = order.shape[1]
    seq = lax.axis_index("seq")
    scale = 1.0 / math.sqrt(NOPE + ROPE)

    def note(i, carry):
        inv[order[0, i]] = i
        return carry

    lax.fori_loop(0, blocks, note, 0)
    seg = seg_rows[...]
    starts = [jnp.sum((seg < v).astype(jnp.int32)) for v in (1, 2, 3)]

    def start_of(label):
        return jnp.where(
            label == 0, 0, jnp.where(label == 1, starts[0], jnp.where(label == 2, starts[1], starts[2]))
        )

    for qb in range(2):
        p = order[0, 2 * seq + qb]
        begin = start_of(segs[0, p * BLK])
        low = begin // BLK
        count = (p - low + 2) // 2
        label_row = seg_rows[pl.ds(p, 1), :]
        start_row = start_of(label_row)
        qpos = lax.broadcasted_iota(jnp.int32, (1, BLK), 1) + p * BLK
        m_ref[...] = jnp.full_like(m_ref, masked_value)
        l_ref[...] = jnp.zeros_like(l_ref)
        acc[...] = jnp.zeros_like(acc)

        def step(i, carry):
            ja = p - 2 * i
            jb = ja - 1
            ra = pl.multiple_of(inv[ja] * BLK, BLK)
            rb = pl.multiple_of(inv[jnp.maximum(jb, 0)] * BLK, BLK)
            kin = lax.broadcasted_iota(jnp.int32, (BLK, BLK), 0)
            kpos = jnp.concatenate([kin + ja * BLK, kin + jb * BLK], axis=0)
            bias = jnp.where((kpos >= start_row) & (kpos <= qpos), 0.0, masked_value)
            kr = jnp.concatenate([kr_ref[pl.ds(ra, BLK), :], kr_ref[pl.ds(rb, BLK), :]], axis=0)
            for h in range(heads):
                cols = slice(h * 128, (h + 1) * 128)
                kn = jnp.concatenate(
                    [k_ref[pl.ds(ra, BLK), cols], k_ref[pl.ds(rb, BLK), cols]], axis=0
                )
                s = lax.dot_general(
                    jnp.concatenate([kn, kr], axis=1),
                    q_ref[h, qb * BLK : (qb + 1) * BLK, :],
                    (((1,), (1,)), ((), ())),
                    preferred_element_type=F32,
                )
                s = s * scale + bias
                old = m_ref[h : h + 1, :]
                new = jnp.maximum(old, jnp.max(s, axis=0, keepdims=True))
                w = jnp.exp(s - new)
                shrink = jnp.exp(old - new)
                m_ref[h : h + 1, :] = new
                l_ref[h : h + 1, :] = l_ref[h : h + 1, :] * shrink + jnp.sum(w, axis=0, keepdims=True)
                vt = jnp.concatenate(
                    [vt_ref[cols, pl.ds(ra, BLK)], vt_ref[cols, pl.ds(rb, BLK)]], axis=1
                )
                acc[h] = acc[h] * shrink + jnp.dot(vt, w.astype(BF16), preferred_element_type=F32)
            return carry

        lax.fori_loop(0, count, step, 0)
        for h in range(heads):
            out_ref[0, qb * BLK : (qb + 1) * BLK, h * VD : (h + 1) * VD] = (
                (acc[h] / l_ref[h : h + 1, :]).T.astype(BF16)
            )
        if qb == 0:
            max_ref[...] = m_ref[...]
        else:
            max_ref[...] = jnp.maximum(max_ref[...], m_ref[...])


def exchange_kernel(nseq, ndp, max_ref, out_ref, mine, got, ssem, rsem, lsem):
    seq, dp = lax.axis_index("seq"), lax.axis_index("dp")
    own = pltpu.make_async_copy(max_ref, mine, lsem.at[0])
    own.start()
    barrier = pltpu.get_barrier_semaphore()
    peers = []
    for n in range(1, nseq * ndp):
        ds, dd = n % nseq, n // nseq
        peers.append({"seq": lax.rem(seq + ds, nseq), "dp": lax.rem(dp + dd, ndp)})
    for peer in peers:
        pl.semaphore_signal(barrier, inc=1, device_id=peer, device_id_type=MESH)
    own.wait()
    pl.semaphore_wait(barrier, len(peers))
    sends = []
    for n, peer in enumerate(peers):
        cp = pltpu.make_async_remote_copy(
            src_ref=mine, dst_ref=got.at[n], send_sem=ssem.at[n], recv_sem=rsem.at[n],
            device_id=peer, device_id_type=MESH,
        )
        cp.start()
        sends.append(cp)
    best = mine[...]
    for n, cp in enumerate(sends):
        cp.wait_recv()
        best = jnp.maximum(best, got[n])
    out_ref[...] = best
    for cp in sends:
        cp.wait_send()


def on_device(nseq, ndp, query_latent, key_latent, rope_key, w_uq, w_uk, w_uv, block_order, segment_ids):
    heads = w_uq.shape[1] // (NOPE + ROPE)
    tokens = key_latent.shape[1]
    total = tokens * nseq
    vmem, anyw, smem = (
        pl.BlockSpec(memory_space=pltpu.VMEM),
        pl.BlockSpec(memory_space=pl.ANY),
        pl.BlockSpec(memory_space=pltpu.SMEM),
    )
    k_all, vt_all, kr_all, q_all = pl.pallas_call(
        gather_kernel,
        out_shape=(
            pltpu.VMEM((total, heads * NOPE), BF16),
            pltpu.VMEM((heads * VD, total), BF16),
            pltpu.VMEM((total, 2 * ROPE), BF16),
            pltpu.VMEM((heads, tokens, 256), BF16),
        ),
        in_specs=[smem, vmem, vmem, anyw, anyw, anyw, anyw],
        out_specs=(vmem, vmem, vmem, vmem),
        scratch_shapes=[
            pltpu.VMEM((nseq, *w_uq.shape), BF16),
            pltpu.VMEM((nseq, *w_uk.shape), BF16),
            pltpu.VMEM((nseq, *w_uv.shape), BF16),
            pltpu.VMEM((NTP, 2, NZ, BLK, 2 * key_latent.shape[2]), BF16),
            pltpu.VMEM((2, NZ, BLK, 2 * ROPE), BF16),
            pltpu.VMEM((NTP, tokens, query_latent.shape[2]), BF16),
            pltpu.VMEM((w_uv.shape[1], nseq * w_uv.shape[0]), BF16),
            pltpu.VMEM((2, tokens, 2 * ROPE), F32),
            pltpu.SemaphoreType.DMA((160,)),
            pltpu.SemaphoreType.DMA((160,)),
            pltpu.SemaphoreType.DMA((4,)),
        ],
        compiler_params=pltpu.CompilerParams(
            collective_id=0, has_side_effects=True, vmem_limit_bytes=40 * MIB
        ),
        name="gather",
    )(block_order, rope_key, key_latent, query_latent, w_uq, w_uk, w_uv)
    context, row_max = pl.pallas_call(
        attention_kernel,
        out_shape=(
            jax.ShapeDtypeStruct((1, tokens, heads * VD), BF16),
            jax.ShapeDtypeStruct((heads, BLK), F32),
        ),
        in_specs=[smem, smem, vmem, vmem, vmem, vmem, vmem],
        out_specs=(vmem, vmem),
        scratch_shapes=[
            pltpu.SMEM((block_order.shape[1],), jnp.int32),
            pltpu.VMEM((heads, VD, BLK), F32),
            pltpu.VMEM((heads, BLK), F32),
            pltpu.VMEM((heads, BLK), F32),
        ],
        compiler_params=pltpu.CompilerParams(vmem_limit_bytes=32 * MIB),
        name="attend",
    )(
        block_order, segment_ids, segment_ids.reshape(-1, BLK),
        q_all, k_all, vt_all, kr_all,
    )
    n = nseq * ndp - 1
    best = pl.pallas_call(
        functools.partial(exchange_kernel, nseq, ndp),
        out_shape=jax.ShapeDtypeStruct((heads, BLK), F32),
        in_specs=[anyw],
        out_specs=vmem,
        scratch_shapes=[
            pltpu.VMEM((heads, BLK), F32),
            pltpu.VMEM((n, heads, BLK), F32),
            pltpu.SemaphoreType.DMA((n,)),
            pltpu.SemaphoreType.DMA((n,)),
            pltpu.SemaphoreType.DMA((1,)),
        ],
        compiler_params=pltpu.CompilerParams(collective_id=1, has_side_effects=True),
        name="exchange",
    )(row_max)
    head_max = jnp.max(best, axis=1)
    ratio = CLIP / jnp.maximum(head_max, CLIP)
    root = jnp.sqrt(ratio)
    factors = jnp.concatenate(
        [
            jnp.broadcast_to(root[:, None], (heads, NOPE)),
            jnp.broadcast_to(ratio[:, None], (heads, ROPE)),
        ],
        axis=1,
    ).reshape(heads * (NOPE + ROPE))
    clipped_uq = (w_uq.astype(F32) * factors[None, :]).astype(BF16)
    clipped_uk = (w_uk.astype(F32) * jnp.repeat(root, NOPE)[None, :]).astype(BF16)
    return (context, clipped_uq, clipped_uk)


def solution(mesh):
    placed = (
        P("dp", "seq", "tp"),
        P("dp", "seq", "tp"),
        P("dp", "seq", None),
        P("seq", "tp"),
        P("seq", "tp"),
        P("seq", "tp"),
        P("dp", None),
        P("dp", None),
    )
    return jax.shard_map(
        functools.partial(on_device, mesh.shape["seq"], mesh.shape["dp"]),
        mesh=mesh,
        in_specs=placed,
        out_specs=(P("dp", "seq", "tp"), P("seq", "tp"), P("seq", "tp")),
        check_vma=False,
    )
```

```python
import functools
import math

import jax
import jax.numpy as jnp
from jax import lax
from jax.experimental import pallas as pl
from jax.experimental.pallas import tpu as pltpu
from jax.sharding import PartitionSpec as P

NOPE = 128
ROPE = 64
VD = 128
CLIP = 8
NZ = 8
NY = 4
NX = 2
NTP = NX * NY
BLK = 128
RUN = 4
MIB = 1 << 20

rope_base = 50000.0
masked_value = -1e30
MESH = pl.DeviceIdType.MESH
F32 = jnp.float32
BF16 = jnp.bfloat16


def cos_sin(angle):
    k = jnp.floor(angle * (2.0 / math.pi) + 0.5)
    r = angle - k * 1.5703125
    r = r - k * 4.837512969970703125e-4
    r = r - k * 7.54978995489188216e-8
    z = r * r
    s = ((-1.9515295891e-4 * z + 8.3321608736e-3) * z - 1.6666654611e-1) * z * r + r
    c = (
        ((2.443315711809948e-5 * z - 1.388731625493765e-3) * z + 4.166664568298827e-2) * z * z
        - 0.5 * z
        + 1.0
    )
    q = k - 4.0 * jnp.floor(k * 0.25)
    odd = (q == 1.0) | (q == 3.0)
    sine = jnp.where(odd, c, s)
    cosine = jnp.where(odd, s, c)
    sine = jnp.where(q >= 2.0, -sine, sine)
    cosine = jnp.where((q == 1.0) | (q == 2.0), -cosine, cosine)
    return cosine, sine


def turning(pos):
    step = lax.broadcasted_iota(jnp.int32, pos.shape, 0).astype(F32) * (2.0 / ROPE)
    return cos_sin(pos.astype(F32) * jnp.exp(-math.log(rope_base) * step))


def rotated(x, cosine, sine):
    a, b = x[: ROPE // 2], x[ROPE // 2 :]
    return jnp.concatenate([a * cosine - b * sine, b * cosine + a * sine], axis=0)


def gather_kernel(
    order, rope_ref, key_hbm, query_hbm, uq_hbm, uk_hbm, uv_hbm,
    k_out, vt_out, kr_out, q_out,
    wq, wk, wv, lp, rr, qg, wvt, trig, ssem, rsem, lsem,
):
    seq = lax.axis_index("seq")
    tp = lax.axis_index("tp")
    z, c = seq // 2, lax.rem(seq, 2)
    x, y = tp // NY, lax.rem(tp, NY)
    oc = 1 - c

    def zmod(d):
        return lax.rem(z + (d + NZ), NZ)

    def col(dx, dy):
        return (x if dx == 0 else 1 - x) * NY + lax.rem(y + (dy + NY), NY)

    right = {"seq": zmod(1) * 2 + c}
    left = {"seq": zmod(-1) * 2 + c}
    sibling = {"seq": z * 2 + oc}
    xside = {"tp": col(1, 0)}
    yup = {"tp": col(0, 1)}
    ydown = {"tp": col(0, -1)}
    offs = (0, -1, 1, -2, 2, -3, 3, 4)

    local = [
        pltpu.make_async_copy(key_hbm.at[0], lp.at[tp, c, 0], lsem.at[4]),
        pltpu.make_async_copy(query_hbm.at[0], qg.at[tp], lsem.at[0]),
        pltpu.make_async_copy(uk_hbm, wk.at[seq], lsem.at[1]),
        pltpu.make_async_copy(uv_hbm, wv.at[seq], lsem.at[2]),
        pltpu.make_async_copy(uq_hbm, wq.at[seq], lsem.at[3]),
    ]
    for cp in local:
        cp.start()
    barrier = pltpu.get_barrier_semaphore()
    for peer in (right, left, sibling, xside, yup, ydown):
        pl.semaphore_signal(barrier, inc=1, device_id=peer, device_id_type=MESH)

    lane = lax.broadcasted_iota(jnp.int32, (ROPE // 2, 2 * BLK), 1)
    p0, p1 = order[0, 2 * seq] * BLK, order[0, 2 * seq + 1] * BLK
    cosine, sine = turning(jnp.where(lane < BLK, p0 + lane, p1 + (lane - BLK)))
    trig[0] = cosine
    trig[1] = sine
    rr[c, z] = rotated(rope_ref[0].astype(F32), cosine, sine).astype(BF16)

    sends = []
    names = {}

    def sem_of(key):
        if key not in names:
            names[key] = len(names)
        return rsem.at[names[key]]

    def send(src, dst, key, peer):
        cp = pltpu.make_async_remote_copy(
            src_ref=src, dst_ref=dst, send_sem=ssem.at[len(sends)], recv_sem=sem_of(key),
            device_id=peer, device_id_type=MESH,
        )
        cp.start()
        sends.append(cp)

    def arrived(ref, key):
        pltpu.make_async_remote_copy(
            src_ref=ref, dst_ref=ref, send_sem=ssem.at[0], recv_sem=sem_of(key),
            device_id=sibling, device_id_type=MESH,
        ).wait_recv()

    half = wq.shape[1] // 2

    def piece(item, sid, core):
        zs = zmod(offs[sid])
        if item == "l":
            return lp.at[tp, core, sid]
        if item == "r":
            return rr.at[core, zs]
        if item == "k":
            return wk.at[zs * 2 + core]
        if item == "v":
            return wv.at[zs * 2 + core]
        return wq.at[zs * 2 + core, pl.ds(half * int(item[1]), half)]

    def moved(item, sid, going):
        if item == "l":
            nxt = {0: 1, 1: 3, 3: 5, 5: 7} if going == "r" else {0: 2, 2: 4, 4: 6, 6: 7}
            return lp.at[tp, c, nxt[sid]], nxt[sid]
        nxt = {0: 1, 1: 3, 3: 5, 5: 7} if going == "r" else {0: 2, 2: 4, 4: 6, 6: 7}
        return piece(item, sid, c), nxt[sid]

    by_right = ("l", "r", "k", "q0")

    def pass_on(item, sid):
        src = piece(item, sid, c)
        if sid in (0, 1, 3) or (sid == 5 and item in by_right):
            dst, n = moved(item, sid, "r")
            send(src, dst, ("ring", item, n), right)
        if sid in (0, 2, 4) or (sid == 6 and item not in by_right):
            dst, n = moved(item, sid, "l")
            send(src, dst, ("ring", item, n), left)
        send(src, src, ("sib", item, sid), sibling)

    def ring(item, *sids):
        for sid in sids:
            arrived(piece(item, sid, c), ("ring", item, sid))
            pass_on(item, sid)

    def part(item, column, core=None):
        if item == "Q":
            return qg.at[column]
        return lp.at[column, c if core is None else core, pl.ds(2 * item, 2)]

    def share(item, column, name):
        if item != "Q":
            ref = part(item, column)
            send(ref, ref, ("share", item, name), sibling)

    def plane_own(item):
        ref = part(item, tp)
        send(ref, ref, ("x", item), xside)
        send(ref, ref, ("up", item, 0), yup)
        send(ref, ref, ("down", item, 0), ydown)

    def plane_x(item):
        ref = part(item, col(1, 0))
        arrived(ref, ("x", item))
        send(ref, ref, ("up", item, 1), yup)
        send(ref, ref, ("down", item, 1), ydown)
        share(item, col(1, 0), "x")

    def plane_y(item):
        for k in (0, 1):
            ref = part(item, col(k, -1))
            arrived(ref, ("up", item, k))
            if k == 0:
                send(ref, ref, ("far", item, 0), yup)
            share(item, col(k, -1), ("up", k))
            ref = part(item, col(k, 1))
            arrived(ref, ("down", item, k))
            if k == 1:
                send(ref, ref, ("far", item, 1), ydown)
            share(item, col(k, 1), ("down", k))

    def plane_far(item):
        for k in (0, 1):
            arrived(part(item, col(k, 2)), ("far", item, k))
            share(item, col(k, 2), ("far", k))

    def from_sibling(item):
        for sid in range(NZ):
            arrived(piece(item, sid, oc), ("sib", item, sid))

    def shared(item):
        arrived(part(item, col(1, 0), oc), ("share", item, "x"))
        for k in (0, 1):
            arrived(part(item, col(k, -1), oc), ("share", item, ("up", k)))
            arrived(part(item, col(k, 1), oc), ("share", item, ("down", k)))
            arrived(part(item, col(k, 2), oc), ("share", item, ("far", k)))

    def project(group):
        def one(i, carry):
            core = i // 2
            sid = 2 * group + lax.rem(i, 2)
            d = (sid + 1) // 2
            away = jnp.where(lax.rem(sid, 2) == 0, d, NZ - d)
            zs = lax.rem(z + away, NZ)
            latent = lp[:, core, sid].reshape(-1, 256)
            first = pl.multiple_of((zs * 2 + core) * 256, 256)
            weight = wk[...].reshape(-1, wk.shape[2])
            k_out[pl.ds(first, 256), :] = lax.dot_general(
                latent, weight, (((0,), (0,)), ((), ())), preferred_element_type=F32
            ).astype(BF16)
            vt_out[:, pl.ds(first, 256)] = jnp.dot(
                wvt[...], latent, preferred_element_type=F32
            ).astype(BF16)
            rot = rr[core, zs].astype(F32)
            kr_out[pl.ds(first, 256), :] = jnp.concatenate([rot, jnp.zeros_like(rot)], axis=0).T.astype(BF16)
            return carry

        lax.fori_loop(0, 4, one, 0)

    pl.semaphore_wait(barrier, 6)
    local[0].wait()
    for item in ("l", "r"):
        pass_on(item, 0)
    local[1].wait()
    plane_own("Q")
    local[2].wait()
    local[3].wait()
    for item in ("k", "v"):
        pass_on(item, 0)
    local[4].wait()
    ring("l", 1, 2)
    ring("r", 1, 2)
    plane_own(0)
    plane_x("Q")
    ring("k", 1, 2)
    ring("v", 1, 2)
    for item in ("q0", "q1"):
        pass_on(item, 0)
    ring("l", 3, 4)
    ring("r", 3, 4)
    plane_own(1)
    plane_x(0)
    plane_y("Q")
    ring("k", 3, 4)
    ring("v", 3, 4)
    ring("l", 5, 6)
    ring("r", 5, 6)
    plane_own(2)
    plane_x(1)
    ring("q0", 1, 2)
    ring("q1", 1, 2)
    plane_y(0)
    ring("l", 7)
    ring("r", 7)
    plane_own(3)
    plane_x(2)
    plane_far("Q")
    ring("k", 5, 6)
    ring("v", 5, 6)
    plane_y(1)
    plane_far(0)
    plane_x(3)
    ring("k", 7)
    ring("v", 7)
    ring("q0", 3, 4)
    ring("q1", 3, 4)
    plane_y(2)
    plane_far(1)
    for item in ("l", "r", "k", "v"):
        from_sibling(item)
    wvt[...] = wv[...].reshape(-1, wv.shape[2]).astype(F32).T.astype(BF16)
    shared(0)
    project(0)
    plane_y(3)
    plane_far(2)
    ring("q0", 5, 6)
    ring("q1", 5, 6)
    shared(1)
    project(1)
    plane_far(3)
    shared(2)
    project(2)
    ring("q0", 7)
    ring("q1", 7)
    shared(3)
    project(3)
    from_sibling("q0")
    from_sibling("q1")

    query = qg[...].reshape(-1, 256)

    def heads_pair(pair, carry):
        cols = pl.ds(pl.multiple_of(pair * 384, 128), 384)
        acc = lax.dot_general(
            wq[:, :, cols].reshape(-1, 384), query, (((0,), (0,)), ((), ())), preferred_element_type=F32
        )
        for b in (0, 1):
            one = acc[b * (NOPE + ROPE) : (b + 1) * (NOPE + ROPE)]
            q_out[2 * pair + b, :NOPE] = one[:NOPE].astype(BF16)
            q_out[2 * pair + b, NOPE : NOPE + ROPE] = rotated(one[NOPE:], trig[0], trig[1]).astype(BF16)
            q_out[2 * pair + b, NOPE + ROPE :] = jnp.zeros((ROPE, 256), BF16)
        return carry

    lax.fori_loop(0, 4, heads_pair, 0)
    for cp in sends:
        cp.wait_send()


def attention_kernel(
    order, segs, seg_rows, q_ref, k_ref, vt_ref, kr_ref, out_ref, max_ref,
    inv, rows, needed, bias, scores, weights, acc,
):
    heads, _, wide = q_ref.shape
    blocks = order.shape[1]
    seq = lax.axis_index("seq")
    scale = 1.0 / math.sqrt(NOPE + ROPE)
    log2 = scale / math.log(2.0)

    def note(i, carry):
        inv[order[0, i]] = i * BLK
        return carry

    lax.fori_loop(0, blocks, note, 0)
    seg = seg_rows[...]
    starts = [jnp.sum((seg < v).astype(jnp.int32)) for v in (1, 2, 3)]

    def start_of(label):
        return jnp.where(
            label == 0, 0, jnp.where(label == 1, starts[0], jnp.where(label == 2, starts[1], starts[2]))
        )

    p = [order[0, 2 * seq + qb] for qb in (0, 1)]
    low = [start_of(segs[0, p[qb] * BLK]) // BLK for qb in (0, 1)]

    def choose(j, n):
        use = ((j >= low[0]) & (j <= p[0])) | ((j >= low[1]) & (j <= p[1]))
        needed[n] = j
        rows[n] = inv[j]
        return n + use.astype(jnp.int32)

    n = lax.fori_loop(0, blocks, choose, 0)
    for extra in range(RUN - 1):
        needed[n + extra] = -1
        rows[n + extra] = 0
    count = (n + RUN - 1) // RUN
    start_row = jnp.concatenate([start_of(seg_rows[pl.ds(p[qb], 1), :]) for qb in (0, 1)], axis=1)
    lanes = lax.broadcasted_iota(jnp.int32, (1, BLK), 1)
    qpos = jnp.concatenate([lanes + p[0] * BLK, lanes + p[1] * BLK], axis=1)

    def mask(i, carry):
        inside = lax.broadcasted_iota(jnp.int32, (BLK, wide), 0)
        for b in range(RUN):
            kpos = inside + needed[RUN * i + b] * BLK
            bias[i, b * BLK : (b + 1) * BLK] = jnp.where(
                (kpos >= start_row) & (kpos <= qpos), 0.0, masked_value
            )
        return carry

    lax.fori_loop(0, count, mask, 0)

    def spot(i):
        return [pl.multiple_of(rows[RUN * i + b], BLK) for b in range(RUN)]

    def score(h, i, top):
        cols = slice(h * NOPE, (h + 1) * NOPE)
        keys = jnp.concatenate(
            [
                jnp.concatenate([k_ref[pl.ds(r, BLK), cols], kr_ref[pl.ds(r, BLK), :]], axis=1)
                for r in spot(i)
            ],
            axis=0,
        )
        s = jnp.dot(keys, q_ref[h], preferred_element_type=F32) + bias[i]
        scores[h % 4, i] = s
        return jnp.maximum(top, jnp.max(s.reshape(-1, 8, wide), axis=0))

    def weigh(h, i, top, total):
        w = jnp.exp2((scores[h % 4, i] - top) * log2)
        weights[h % 4, i] = w.astype(BF16)
        return total + jnp.sum(w.reshape(-1, 8, wide), axis=0)

    def mix(h, i):
        cols = slice(h * VD, (h + 1) * VD)
        values = jnp.concatenate([vt_ref[cols, pl.ds(r, BLK)] for r in spot(i)], axis=1)
        acc[h % 2] += jnp.dot(values, weights[h % 4, i], preferred_element_type=F32)

    low_top = jnp.full((8, wide), masked_value, F32)
    zero = jnp.zeros((8, wide), F32)
    tops, totals, sums = {}, {}, {}
    for stage in range(0, heads + 4, 2):
        scored = [h for h in (stage, stage + 1) if h < heads]
        weighed = [h for h in (stage - 2, stage - 1) if 0 <= h < heads]
        mixed = [h for h in (stage - 4, stage - 3) if 0 <= h < heads]
        for h in weighed:
            tops[h] = jnp.max(tops[h], axis=0, keepdims=True)
            max_ref[h : h + 1, :] = jnp.maximum(tops[h][:, :BLK], tops[h][:, BLK:]) * scale
        if mixed:
            acc[...] = jnp.zeros_like(acc)

        def body(i, carry):
            found, added = carry
            for h in mixed:
                mix(h, i)
            added = [weigh(h, i, tops[h], t) for h, t in zip(weighed, added)]
            found = [score(h, i, t) for h, t in zip(scored, found)]
            return found, added

        found, added = lax.fori_loop(
            0, count, body, ([low_top for h in scored], [zero for h in weighed])
        )
        tops.update(zip(scored, found))
        totals.update(zip(weighed, added))
        for h in mixed:
            total = jnp.sum(totals[h], axis=0, keepdims=True)
            out_ref[0, :, h * VD : (h + 1) * VD] = (acc[h % 2] / total).T.astype(BF16)


def attend(block_order, segment_ids, q_all, k_all, vt_all, kr_all):
    heads, _, tokens = q_all.shape
    vmem, smem = pl.BlockSpec(memory_space=pltpu.VMEM), pl.BlockSpec(memory_space=pltpu.SMEM)
    return pl.pallas_call(
        attention_kernel,
        out_shape=(
            jax.ShapeDtypeStruct((1, tokens, heads * VD), BF16),
            jax.ShapeDtypeStruct((heads, BLK), F32),
        ),
        in_specs=[smem, smem, vmem, vmem, vmem, vmem, vmem],
        out_specs=(vmem, vmem),
        scratch_shapes=[
            pltpu.SMEM((block_order.shape[1],), jnp.int32),
            pltpu.SMEM((block_order.shape[1] + 8,), jnp.int32),
            pltpu.SMEM((block_order.shape[1] + 8,), jnp.int32),
            pltpu.VMEM((block_order.shape[1] // RUN, RUN * BLK, tokens), F32),
            pltpu.VMEM((4, block_order.shape[1] // RUN, RUN * BLK, tokens), F32),
            pltpu.VMEM((4, block_order.shape[1] // RUN, RUN * BLK, tokens), BF16),
            pltpu.VMEM((2, VD, tokens), F32),
        ],
        compiler_params=pltpu.CompilerParams(vmem_limit_bytes=40 * MIB),
        name="attend",
    )(
        block_order, segment_ids, segment_ids.reshape(-1, BLK),
        *(pltpu.with_memory_space_constraint(v, pltpu.VMEM) for v in (q_all, k_all, vt_all, kr_all)),
    )


def exchange_kernel(nseq, ndp, max_ref, out_ref, mine, got, ssem, rsem, lsem):
    seq, dp = lax.axis_index("seq"), lax.axis_index("dp")
    own = pltpu.make_async_copy(max_ref, mine, lsem.at[0])
    own.start()
    barrier = pltpu.get_barrier_semaphore()
    peers = []
    for n in range(1, nseq * ndp):
        ds, dd = n % nseq, n // nseq
        peers.append({"seq": lax.rem(seq + ds, nseq), "dp": lax.rem(dp + dd, ndp)})
    for peer in peers:
        pl.semaphore_signal(barrier, inc=1, device_id=peer, device_id_type=MESH)
    own.wait()
    pl.semaphore_wait(barrier, len(peers))
    sends = []
    for n, peer in enumerate(peers):
        cp = pltpu.make_async_remote_copy(
            src_ref=mine, dst_ref=got.at[n], send_sem=ssem.at[n], recv_sem=rsem.at[n],
            device_id=peer, device_id_type=MESH,
        )
        cp.start()
        sends.append(cp)
    best = mine[...]
    for n, cp in enumerate(sends):
        cp.wait_recv()
        best = jnp.maximum(best, got[n])
    out_ref[...] = best
    for cp in sends:
        cp.wait_send()


def on_device(nseq, ndp, query_latent, key_latent, rope_key, w_uq, w_uk, w_uv, block_order, segment_ids):
    heads = w_uq.shape[1] // (NOPE + ROPE)
    tokens = key_latent.shape[1]
    total = tokens * nseq
    vmem, anyw, smem = (
        pl.BlockSpec(memory_space=pltpu.VMEM),
        pl.BlockSpec(memory_space=pl.ANY),
        pl.BlockSpec(memory_space=pltpu.SMEM),
    )
    k_all, vt_all, kr_all, q_all = pl.pallas_call(
        gather_kernel,
        out_shape=(
            pltpu.VMEM((total, heads * NOPE), BF16),
            pltpu.VMEM((heads * VD, total), BF16),
            pltpu.VMEM((total, 2 * ROPE), BF16),
            pltpu.VMEM((heads, 256, tokens), BF16),
        ),
        in_specs=[smem, vmem, anyw, anyw, anyw, anyw, anyw],
        out_specs=(vmem, vmem, vmem, vmem),
        scratch_shapes=[
            pltpu.VMEM((nseq, *w_uq.shape), BF16),
            pltpu.VMEM((nseq, *w_uk.shape), BF16),
            pltpu.VMEM((nseq, *w_uv.shape), BF16),
            pltpu.VMEM((NTP, 2, NZ, key_latent.shape[2], tokens), BF16),
            pltpu.VMEM((2, NZ, ROPE, tokens), BF16),
            pltpu.VMEM((NTP, query_latent.shape[2], tokens), BF16),
            pltpu.VMEM((w_uv.shape[1], nseq * w_uv.shape[0]), BF16),
            pltpu.VMEM((2, ROPE // 2, tokens), F32),
            pltpu.SemaphoreType.DMA((160,)),
            pltpu.SemaphoreType.DMA((160,)),
            pltpu.SemaphoreType.DMA((5,)),
        ],
        compiler_params=pltpu.CompilerParams(
            collective_id=0, has_side_effects=True, vmem_limit_bytes=40 * MIB
        ),
        name="gather",
    )(
        block_order, jnp.swapaxes(rope_key, 1, 2), jnp.swapaxes(key_latent, 1, 2),
        jnp.swapaxes(query_latent, 1, 2), w_uq, w_uk, w_uv,
    )
    context, row_max = attend(block_order, segment_ids, q_all, k_all, vt_all, kr_all)
    n = nseq * ndp - 1
    best = pl.pallas_call(
        functools.partial(exchange_kernel, nseq, ndp),
        out_shape=jax.ShapeDtypeStruct((heads, BLK), F32),
        in_specs=[anyw],
        out_specs=vmem,
        scratch_shapes=[
            pltpu.VMEM((heads, BLK), F32),
            pltpu.VMEM((n, heads, BLK), F32),
            pltpu.SemaphoreType.DMA((n,)),
            pltpu.SemaphoreType.DMA((n,)),
            pltpu.SemaphoreType.DMA((1,)),
        ],
        compiler_params=pltpu.CompilerParams(collective_id=1, has_side_effects=True),
        name="exchange",
    )(row_max)
    head_max = jnp.max(best, axis=1)
    ratio = CLIP / jnp.maximum(head_max, CLIP)
    root = jnp.sqrt(ratio)
    factors = jnp.concatenate(
        [
            jnp.broadcast_to(root[:, None], (heads, NOPE)),
            jnp.broadcast_to(ratio[:, None], (heads, ROPE)),
        ],
        axis=1,
    ).reshape(heads * (NOPE + ROPE))
    clipped_uq = (w_uq.astype(F32) * factors[None, :]).astype(BF16)
    clipped_uk = (w_uk.astype(F32) * jnp.repeat(root, NOPE)[None, :]).astype(BF16)
    return (context, clipped_uq, clipped_uk)


def solution(mesh):
    placed = (
        P("dp", "seq", "tp"),
        P("dp", "seq", "tp"),
        P("dp", "seq", None),
        P("seq", "tp"),
        P("seq", "tp"),
        P("seq", "tp"),
        P("dp", None),
        P("dp", None),
    )
    return jax.shard_map(
        functools.partial(on_device, mesh.shape["seq"], mesh.shape["dp"]),
        mesh=mesh,
        in_specs=placed,
        out_specs=(P("dp", "seq", "tp"), P("seq", "tp"), P("seq", "tp")),
        check_vma=False,
    )
```

```python
import functools
import math

import jax
import jax.numpy as jnp
from jax import lax
from jax.experimental import pallas as pl
from jax.experimental.pallas import tpu as pltpu
from jax.sharding import PartitionSpec as P

NOPE = 128
ROPE = 64
VD = 128
CLIP = 8
NZ = 8
NY = 4
NX = 2
NTP = NX * NY
BLK = 128
RUN = 4
MIB = 1 << 20

rope_base = 50000.0
masked_value = -1e30
MESH = pl.DeviceIdType.MESH
F32 = jnp.float32
BF16 = jnp.bfloat16


def cos_sin(angle):
    k = jnp.floor(angle * (2.0 / math.pi) + 0.5)
    r = angle - k * 1.5703125
    r = r - k * 4.837512969970703125e-4
    r = r - k * 7.54978995489188216e-8
    z = r * r
    s = ((-1.9515295891e-4 * z + 8.3321608736e-3) * z - 1.6666654611e-1) * z * r + r
    c = (
        ((2.443315711809948e-5 * z - 1.388731625493765e-3) * z + 4.166664568298827e-2) * z * z
        - 0.5 * z
        + 1.0
    )
    q = k - 4.0 * jnp.floor(k * 0.25)
    odd = (q == 1.0) | (q == 3.0)
    sine = jnp.where(odd, c, s)
    cosine = jnp.where(odd, s, c)
    sine = jnp.where(q >= 2.0, -sine, sine)
    cosine = jnp.where((q == 1.0) | (q == 2.0), -cosine, cosine)
    return cosine, sine


def turning(pos):
    step = lax.broadcasted_iota(jnp.int32, pos.shape, 0).astype(F32) * (2.0 / ROPE)
    return cos_sin(pos.astype(F32) * jnp.exp(-math.log(rope_base) * step))


def rotated(x, cosine, sine):
    a, b = x[: ROPE // 2], x[ROPE // 2 :]
    return jnp.concatenate([a * cosine - b * sine, b * cosine + a * sine], axis=0)


def gather_kernel(
    order, rope_ref, key_hbm, query_hbm, uq_hbm, uk_hbm, uv_hbm,
    k_out, vt_out, kr_out, q_out,
    wq, wk, wv, lp, rr, qg, wvt, trig, ssem, rsem, lsem,
):
    seq = lax.axis_index("seq")
    tp = lax.axis_index("tp")
    dp = lax.axis_index("dp")
    z, c = seq // 2, lax.rem(seq, 2)
    x, y = tp // NY, lax.rem(tp, NY)
    oc = 1 - c

    def zmod(d):
        return lax.rem(z + (d + NZ), NZ)

    def col(dx, dy):
        return (x if dx == 0 else 1 - x) * NY + lax.rem(y + (dy + NY), NY)

    right = {"seq": zmod(1) * 2 + c}
    left = {"seq": zmod(-1) * 2 + c}
    sibling = {"seq": z * 2 + oc}
    xside = {"tp": col(1, 0)}
    yup = {"tp": col(0, 1)}
    ydown = {"tp": col(0, -1)}
    twin = {"dp": 1 - dp}
    offs = (0, -1, 1, -2, 2, -3, 3, 4)

    local = [
        pltpu.make_async_copy(key_hbm.at[0], lp.at[tp, c, 0], lsem.at[4]),
        pltpu.make_async_copy(query_hbm.at[0], qg.at[tp], lsem.at[0]),
        pltpu.make_async_copy(uk_hbm, wk.at[seq], lsem.at[1]),
        pltpu.make_async_copy(uv_hbm, wv.at[seq], lsem.at[2]),
        pltpu.make_async_copy(uq_hbm, wq.at[seq], lsem.at[3]),
    ]
    for cp in local:
        cp.start()
    barrier = pltpu.get_barrier_semaphore()
    for peer in (right, left, sibling, xside, yup, ydown, twin):
        pl.semaphore_signal(barrier, inc=1, device_id=peer, device_id_type=MESH)

    lane = lax.broadcasted_iota(jnp.int32, (ROPE // 2, 2 * BLK), 1)
    p0, p1 = order[0, 2 * seq] * BLK, order[0, 2 * seq + 1] * BLK
    cosine, sine = turning(jnp.where(lane < BLK, p0 + lane, p1 + (lane - BLK)))
    trig[0] = cosine
    trig[1] = sine
    rr[c, z] = rotated(rope_ref[0].astype(F32), cosine, sine).astype(BF16)

    sends = []
    names = {}

    def sem_of(key):
        if key not in names:
            names[key] = len(names)
        return rsem.at[names[key]]

    def send(src, dst, key, peer):
        cp = pltpu.make_async_remote_copy(
            src_ref=src, dst_ref=dst, send_sem=ssem.at[len(sends)], recv_sem=sem_of(key),
            device_id=peer, device_id_type=MESH,
        )
        cp.start()
        sends.append(cp)

    def arrived(ref, key):
        pltpu.make_async_remote_copy(
            src_ref=ref, dst_ref=ref, send_sem=ssem.at[0], recv_sem=sem_of(key),
            device_id=sibling, device_id_type=MESH,
        ).wait_recv()

    half = wq.shape[1] // 2

    def piece(item, sid, core, side=dp):
        zs = zmod(offs[sid])
        if item == "l":
            return lp.at[tp, core, sid]
        if item == "r":
            return rr.at[core, zs]
        if item == "k":
            return wk.at[zs * 2 + core]
        if item == "v":
            return wv.at[zs * 2 + core]
        return wq.at[zs * 2 + core, pl.ds(pl.multiple_of(half * side, half), half)]

    onward = {"r": {0: 1, 1: 3, 3: 5, 5: 7}, "l": {0: 2, 2: 4, 4: 6, 6: 7}}

    def moved(item, sid, going):
        nxt = onward[going][sid]
        return (lp.at[tp, c, nxt] if item == "l" else piece(item, sid, c)), nxt

    def pass_on(item, sid):
        src = piece(item, sid, c)
        if sid in (0, 1, 3) or (sid == 5 and item != "q"):
            dst, n = moved(item, sid, "r")
            send(src, dst, ("ring", item, n), right)
        if sid in (0, 2, 4) or (sid == 6 and item == "q"):
            dst, n = moved(item, sid, "l")
            send(src, dst, ("ring", item, n), left)
        if item == "q" and sid > 0:
            send(src, src, ("twin", sid), twin)
        if item == "q" and sid == 0:
            src = wq.at[seq]
        send(src, src, ("sib", item, sid), sibling)

    def ring(item, *sids):
        for sid in sids:
            arrived(piece(item, sid, c), ("ring", item, sid))
            pass_on(item, sid)

    def from_twin(*sids):
        for sid in sids:
            ref = piece("q", sid, c, 1 - dp)
            arrived(ref, ("twin", sid))
            send(ref, ref, ("twinsib", sid), sibling)

    def queries_of_sibling():
        arrived(wq.at[z * 2 + oc], ("sib", "q", 0))
        for sid in range(1, NZ):
            arrived(piece("q", sid, oc), ("sib", "q", sid))
            arrived(piece("q", sid, oc, 1 - dp), ("twinsib", sid))

    def part(item, column, core=None):
        if item == "Q":
            return qg.at[column]
        return lp.at[column, c if core is None else core, pl.ds(2 * item, 2)]

    def share(item, column, name):
        if item != "Q":
            ref = part(item, column)
            send(ref, ref, ("share", item, name), sibling)

    def plane_own(item):
        ref = part(item, tp)
        send(ref, ref, ("x", item), xside)
        send(ref, ref, ("up", item, 0), yup)
        send(ref, ref, ("down", item, 0), ydown)

    def plane_x(item):
        ref = part(item, col(1, 0))
        arrived(ref, ("x", item))
        send(ref, ref, ("up", item, 1), yup)
        send(ref, ref, ("down", item, 1), ydown)
        share(item, col(1, 0), "x")

    def plane_y(item):
        for k in (0, 1):
            ref = part(item, col(k, -1))
            arrived(ref, ("up", item, k))
            if k == 0:
                send(ref, ref, ("far", item, 0), yup)
            share(item, col(k, -1), ("up", k))
            ref = part(item, col(k, 1))
            arrived(ref, ("down", item, k))
            if k == 1:
                send(ref, ref, ("far", item, 1), ydown)
            share(item, col(k, 1), ("down", k))

    def plane_far(item):
        for k in (0, 1):
            arrived(part(item, col(k, 2)), ("far", item, k))
            share(item, col(k, 2), ("far", k))

    def from_sibling(item):
        for sid in range(NZ):
            arrived(piece(item, sid, oc), ("sib", item, sid))

    def shared(item):
        arrived(part(item, col(1, 0), oc), ("share", item, "x"))
        for k in (0, 1):
            arrived(part(item, col(k, -1), oc), ("share", item, ("up", k)))
            arrived(part(item, col(k, 1), oc), ("share", item, ("down", k)))
            arrived(part(item, col(k, 2), oc), ("share", item, ("far", k)))

    def project(group, keys, values):
        sids = (2 * group, 2 * group + 1)

        def one(core, carry):
            latent = jnp.concatenate([lp[:, core, sid].reshape(-1, 256) for sid in sids], axis=1)
            first = [pl.multiple_of((zmod(offs[sid]) * 2 + core) * 256, 256) for sid in sids]
            if keys:
                weight = wk[...].reshape(-1, wk.shape[2])
                made = lax.dot_general(
                    latent, weight, (((0,), (0,)), ((), ())), preferred_element_type=F32
                ).astype(BF16)
                for n, sid in enumerate(sids):
                    k_out[pl.ds(first[n], 256), :] = made[n * 256 : (n + 1) * 256]
                    rot = rr[core, zmod(offs[sid])].astype(F32)
                    kr_out[pl.ds(first[n], 256), :] = jnp.concatenate(
                        [rot, jnp.zeros_like(rot)], axis=0
                    ).T.astype(BF16)
            if values:
                made = jnp.dot(wvt[...], latent, preferred_element_type=F32).astype(BF16)
                for n in range(2):
                    vt_out[:, pl.ds(first[n], 256)] = made[:, n * 256 : (n + 1) * 256]
            return carry

        lax.fori_loop(0, 2, one, 0)

    pl.semaphore_wait(barrier, 7)
    local[0].wait()
    for item in ("l", "r"):
        pass_on(item, 0)
    local[1].wait()
    plane_own("Q")
    local[2].wait()
    local[3].wait()
    pass_on("k", 0)
    local[4].wait()
    pass_on("q", 0)
    ring("l", 1, 2)
    ring("r", 1, 2)
    plane_own(0)
    ring("k", 1, 2)
    plane_x("Q")
    ring("q", 1, 2)
    ring("l", 3, 4)
    ring("r", 3, 4)
    plane_own(1)
    plane_x(0)
    ring("k", 3, 4)
    plane_y("Q")
    pass_on("v", 0)
    ring("l", 5, 6)
    ring("r", 5, 6)
    plane_own(2)
    plane_x(1)
    ring("k", 5, 6)
    plane_y(0)
    ring("q", 3, 4)
    ring("v", 1, 2)
    ring("l", 7)
    ring("r", 7)
    plane_own(3)
    ring("k", 7)
    plane_x(2)
    plane_far("Q")
    ring("q", 5, 6)
    ring("v", 3, 4)
    plane_y(1)
    plane_far(0)
    from_twin(1, 2)
    for item in ("l", "r", "k"):
        from_sibling(item)
    shared(0)
    ring("v", 5, 6)
    project(0, True, False)
    ring("q", 7)
    plane_x(3)
    plane_y(2)
    plane_far(1)
    ring("v", 7)
    from_twin(3, 4)
    shared(1)
    project(1, True, False)
    from_sibling("v")
    wvt[...] = wv[...].reshape(-1, wv.shape[2]).astype(F32).T.astype(BF16)
    plane_y(3)
    plane_far(2)
    project(0, False, True)
    from_twin(5, 6)
    shared(2)
    project(1, False, True)
    plane_far(3)
    from_twin(7)
    project(2, True, True)
    shared(3)
    project(3, True, True)
    queries_of_sibling()

    query = qg[...].reshape(-1, 256)

    def heads_pair(pair, carry):
        cols = pl.ds(pl.multiple_of(pair * 384, 128), 384)
        acc = lax.dot_general(
            wq[:, :, cols].reshape(-1, 384), query, (((0,), (0,)), ((), ())), preferred_element_type=F32
        )
        for b in (0, 1):
            one = acc[b * (NOPE + ROPE) : (b + 1) * (NOPE + ROPE)]
            q_out[2 * pair + b, :NOPE] = one[:NOPE].astype(BF16)
            q_out[2 * pair + b, NOPE : NOPE + ROPE] = rotated(one[NOPE:], trig[0], trig[1]).astype(BF16)
            q_out[2 * pair + b, NOPE + ROPE :] = jnp.zeros((ROPE, 256), BF16)
        return carry

    lax.fori_loop(0, 4, heads_pair, 0)
    for cp in sends:
        cp.wait_send()


def attention_kernel(
    order, segs, seg_rows, q_ref, k_ref, vt_ref, kr_ref, out_ref, max_ref,
    inv, rows, needed, bias, scores, weights, acc,
):
    heads, _, wide = q_ref.shape
    blocks = order.shape[1]
    seq = lax.axis_index("seq")
    scale = 1.0 / math.sqrt(NOPE + ROPE)
    log2 = scale / math.log(2.0)

    def note(i, carry):
        inv[order[0, i]] = i * BLK
        return carry

    lax.fori_loop(0, blocks, note, 0)
    seg = seg_rows[...]
    starts = [jnp.sum((seg < v).astype(jnp.int32)) for v in (1, 2, 3)]

    def start_of(label):
        return jnp.where(
            label == 0, 0, jnp.where(label == 1, starts[0], jnp.where(label == 2, starts[1], starts[2]))
        )

    p = [order[0, 2 * seq + qb] for qb in (0, 1)]
    low = [start_of(segs[0, p[qb] * BLK]) // BLK for qb in (0, 1)]

    def choose(j, n):
        use = ((j >= low[0]) & (j <= p[0])) | ((j >= low[1]) & (j <= p[1]))
        needed[n] = j
        rows[n] = inv[j]
        return n + use.astype(jnp.int32)

    n = lax.fori_loop(0, blocks, choose, 0)
    for extra in range(RUN - 1):
        needed[n + extra] = -1
        rows[n + extra] = 0
    count = (n + RUN - 1) // RUN
    start_row = jnp.concatenate([start_of(seg_rows[pl.ds(p[qb], 1), :]) for qb in (0, 1)], axis=1)
    lanes = lax.broadcasted_iota(jnp.int32, (1, BLK), 1)
    qpos = jnp.concatenate([lanes + p[0] * BLK, lanes + p[1] * BLK], axis=1)

    def mask(i, carry):
        inside = lax.broadcasted_iota(jnp.int32, (BLK, wide), 0)
        for b in range(RUN):
            kpos = inside + needed[RUN * i + b] * BLK
            bias[i, b * BLK : (b + 1) * BLK] = jnp.where(
                (kpos >= start_row) & (kpos <= qpos), 0.0, masked_value
            )
        return carry

    lax.fori_loop(0, count, mask, 0)

    def spot(i):
        return [pl.multiple_of(rows[RUN * i + b], BLK) for b in range(RUN)]

    def score(h, i, top):
        cols = slice(h * NOPE, (h + 1) * NOPE)
        keys = jnp.concatenate(
            [
                jnp.concatenate([k_ref[pl.ds(r, BLK), cols], kr_ref[pl.ds(r, BLK), :]], axis=1)
                for r in spot(i)
            ],
            axis=0,
        )
        s = jnp.dot(keys, q_ref[h], preferred_element_type=F32) + bias[i]
        scores[h % 4, i] = s
        return jnp.maximum(top, jnp.max(s.reshape(-1, 8, wide), axis=0))

    def weigh(h, i, top, total):
        w = jnp.exp2((scores[h % 4, i] - top) * log2)
        weights[h % 4, i] = w.astype(BF16)
        return total + jnp.sum(w.reshape(-1, 8, wide), axis=0)

    def mix(h, i):
        cols = slice(h * VD, (h + 1) * VD)
        values = jnp.concatenate([vt_ref[cols, pl.ds(r, BLK)] for r in spot(i)], axis=1)
        acc[h % 2] += jnp.dot(values, weights[h % 4, i], preferred_element_type=F32)

    low_top = jnp.full((8, wide), masked_value, F32)
    zero = jnp.zeros((8, wide), F32)
    tops, totals, sums = {}, {}, {}
    for stage in range(0, heads + 4, 2):
        scored = [h for h in (stage, stage + 1) if h < heads]
        weighed = [h for h in (stage - 2, stage - 1) if 0 <= h < heads]
        mixed = [h for h in (stage - 4, stage - 3) if 0 <= h < heads]
        for h in weighed:
            tops[h] = jnp.max(tops[h], axis=0, keepdims=True)
            max_ref[h : h + 1, :] = jnp.maximum(tops[h][:, :BLK], tops[h][:, BLK:]) * scale
        if mixed:
            acc[...] = jnp.zeros_like(acc)

        def body(i, carry):
            found, added = carry
            for h in mixed:
                mix(h, i)
            added = [weigh(h, i, tops[h], t) for h, t in zip(weighed, added)]
            found = [score(h, i, t) for h, t in zip(scored, found)]
            return found, added

        found, added = lax.fori_loop(
            0, count, body, ([low_top for h in scored], [zero for h in weighed])
        )
        tops.update(zip(scored, found))
        totals.update(zip(weighed, added))
        for h in mixed:
            total = jnp.sum(totals[h], axis=0, keepdims=True)
            out_ref[0, :, h * VD : (h + 1) * VD] = (acc[h % 2] / total).T.astype(BF16)


def attend(block_order, segment_ids, q_all, k_all, vt_all, kr_all):
    heads, _, tokens = q_all.shape
    vmem, smem = pl.BlockSpec(memory_space=pltpu.VMEM), pl.BlockSpec(memory_space=pltpu.SMEM)
    return pl.pallas_call(
        attention_kernel,
        out_shape=(
            jax.ShapeDtypeStruct((1, tokens, heads * VD), BF16),
            jax.ShapeDtypeStruct((heads, BLK), F32),
        ),
        in_specs=[smem, smem, vmem, vmem, vmem, vmem, vmem],
        out_specs=(vmem, vmem),
        scratch_shapes=[
            pltpu.SMEM((block_order.shape[1],), jnp.int32),
            pltpu.SMEM((block_order.shape[1] + 8,), jnp.int32),
            pltpu.SMEM((block_order.shape[1] + 8,), jnp.int32),
            pltpu.VMEM((block_order.shape[1] // RUN, RUN * BLK, tokens), F32),
            pltpu.VMEM((4, block_order.shape[1] // RUN, RUN * BLK, tokens), F32),
            pltpu.VMEM((4, block_order.shape[1] // RUN, RUN * BLK, tokens), BF16),
            pltpu.VMEM((2, VD, tokens), F32),
        ],
        compiler_params=pltpu.CompilerParams(
            vmem_limit_bytes=40 * MIB
        ),
        name="attend",
    )(
        block_order, segment_ids, segment_ids.reshape(-1, BLK),
        *(pltpu.with_memory_space_constraint(v, pltpu.VMEM) for v in (q_all, k_all, vt_all, kr_all)),
    )


def exchange_kernel(nseq, ndp, max_ref, out_ref, mine, got, ssem, rsem, lsem):
    seq, dp = lax.axis_index("seq"), lax.axis_index("dp")
    own = pltpu.make_async_copy(max_ref, mine, lsem.at[0])
    own.start()
    barrier = pltpu.get_barrier_semaphore()
    peers = []
    for n in range(1, nseq * ndp):
        ds, dd = n % nseq, n // nseq
        peers.append({"seq": lax.rem(seq + ds, nseq), "dp": lax.rem(dp + dd, ndp)})
    for peer in peers:
        pl.semaphore_signal(barrier, inc=1, device_id=peer, device_id_type=MESH)
    own.wait()
    pl.semaphore_wait(barrier, len(peers))
    sends = []
    for n, peer in enumerate(peers):
        cp = pltpu.make_async_remote_copy(
            src_ref=mine, dst_ref=got.at[n], send_sem=ssem.at[n], recv_sem=rsem.at[n],
            device_id=peer, device_id_type=MESH,
        )
        cp.start()
        sends.append(cp)
    best = mine[...]
    for n, cp in enumerate(sends):
        cp.wait_recv()
        best = jnp.maximum(best, got[n])
    out_ref[...] = best
    for cp in sends:
        cp.wait_send()


def on_device(nseq, ndp, query_latent, key_latent, rope_key, w_uq, w_uk, w_uv, block_order, segment_ids):
    heads = w_uq.shape[1] // (NOPE + ROPE)
    tokens = key_latent.shape[1]
    total = tokens * nseq
    vmem, anyw, smem = (
        pl.BlockSpec(memory_space=pltpu.VMEM),
        pl.BlockSpec(memory_space=pl.ANY),
        pl.BlockSpec(memory_space=pltpu.SMEM),
    )
    k_all, vt_all, kr_all, q_all = pl.pallas_call(
        gather_kernel,
        out_shape=(
            pltpu.VMEM((total, heads * NOPE), BF16),
            pltpu.VMEM((heads * VD, total), BF16),
            pltpu.VMEM((total, 2 * ROPE), BF16),
            pltpu.VMEM((heads, 256, tokens), BF16),
        ),
        in_specs=[smem, vmem, anyw, anyw, anyw, anyw, anyw],
        out_specs=(vmem, vmem, vmem, vmem),
        scratch_shapes=[
            pltpu.VMEM((nseq, *w_uq.shape), BF16),
            pltpu.VMEM((nseq, *w_uk.shape), BF16),
            pltpu.VMEM((nseq, *w_uv.shape), BF16),
            pltpu.VMEM((NTP, 2, NZ, key_latent.shape[2], tokens), BF16),
            pltpu.VMEM((2, NZ, ROPE, tokens), BF16),
            pltpu.VMEM((NTP, query_latent.shape[2], tokens), BF16),
            pltpu.VMEM((w_uv.shape[1], nseq * w_uv.shape[0]), BF16),
            pltpu.VMEM((2, ROPE // 2, tokens), F32),
            pltpu.SemaphoreType.DMA((176,)),
            pltpu.SemaphoreType.DMA((176,)),
            pltpu.SemaphoreType.DMA((5,)),
        ],
        compiler_params=pltpu.CompilerParams(
            collective_id=0, has_side_effects=True, vmem_limit_bytes=40 * MIB
        ),
        name="gather",
    )(
        block_order, jnp.swapaxes(rope_key, 1, 2), jnp.swapaxes(key_latent, 1, 2),
        jnp.swapaxes(query_latent, 1, 2), w_uq, w_uk, w_uv,
    )
    context, row_max = attend(block_order, segment_ids, q_all, k_all, vt_all, kr_all)
    n = nseq * ndp - 1
    best = pl.pallas_call(
        functools.partial(exchange_kernel, nseq, ndp),
        out_shape=jax.ShapeDtypeStruct((heads, BLK), F32),
        in_specs=[anyw],
        out_specs=vmem,
        scratch_shapes=[
            pltpu.VMEM((heads, BLK), F32),
            pltpu.VMEM((n, heads, BLK), F32),
            pltpu.SemaphoreType.DMA((n,)),
            pltpu.SemaphoreType.DMA((n,)),
            pltpu.SemaphoreType.DMA((1,)),
        ],
        compiler_params=pltpu.CompilerParams(collective_id=1, has_side_effects=True),
        name="exchange",
    )(row_max)
    head_max = jnp.max(best, axis=1)
    ratio = CLIP / jnp.maximum(head_max, CLIP)
    root = jnp.sqrt(ratio)
    factors = jnp.concatenate(
        [
            jnp.broadcast_to(root[:, None], (heads, NOPE)),
            jnp.broadcast_to(ratio[:, None], (heads, ROPE)),
        ],
        axis=1,
    ).reshape(heads * (NOPE + ROPE))
    clipped_uq = (w_uq.astype(F32) * factors[None, :]).astype(BF16)
    clipped_uk = (w_uk.astype(F32) * jnp.repeat(root, NOPE)[None, :]).astype(BF16)
    return (context, clipped_uq, clipped_uk)


def solution(mesh):
    placed = (
        P("dp", "seq", "tp"),
        P("dp", "seq", "tp"),
        P("dp", "seq", None),
        P("seq", "tp"),
        P("seq", "tp"),
        P("seq", "tp"),
        P("dp", None),
        P("dp", None),
    )
    return jax.shard_map(
        functools.partial(on_device, mesh.shape["seq"], mesh.shape["dp"]),
        mesh=mesh,
        in_specs=placed,
        out_specs=(P("dp", "seq", "tp"), P("seq", "tp"), P("seq", "tp")),
        check_vma=False,
    )
```
